256 devices in a mesh: data: 32 (over z, y_hi, core), width: 8 (over y_lo, x).
Axes of the slice: x: 4, y: 4 (y_hi: 2, y_lo: 2; y = y_hi * 2 + y_lo), z: 8, core: 2. Of those that a mesh axis runs over, the one named last changes fastest.
Arguments:
- slope_up: float32 [32, 1280, 5120], P('data', None, 'width'), may hold values from -1.25 to 1.25
- slope_down: float32 [32, 5120, 1280], P('data', 'width'), may hold values from -1.25 to 1.25
- slope_query: float32 [32, 1280, 1280], P('data', None, 'width'), may hold values from -1.25 to 1.25
- slope_key: float32 [32, 1280, 1280], P('data', None, 'width'), may hold values from -1.25 to 1.25
- slope_value: float32 [32, 1280, 1280], P('data', None, 'width'), may hold values from -1.25 to 1.25
- slope_mixed: float32 [32, 1280, 1280], P('data', 'width'), may hold values from -1.25 to 1.25
- slope_norm: float32 [32, 1280], P('data'), may hold values from -12 to 12
- slope_bias: float32 [32, 1280], P('data'), may hold values from -12 to 12
- param_up: float32 [1280, 5120], P('data', 'width'), may hold values from -0.15625 to 0.15625
- param_down: float32 [5120, 1280], P('width', 'data'), may hold values from -0.078125 to 0.078125
- param_query: float32 [1280, 1280], P('data', 'width'), may hold values from -0.15625 to 0.15625
- param_key: float32 [1280, 1280], P('data', 'width'), may hold values from -0.15625 to 0.15625
- param_value: float32 [1280, 1280], P('data', 'width'), may hold values from -0.15625 to 0.15625
- param_mixed: float32 [1280, 1280], P('width', 'data'), may hold values from -0.15625 to 0.15625
- param_norm: float32 [1280], P('data'), may hold values from 0.25 to 1.75
- param_bias: float32 [1280], P('data'), may hold values from -3 to 3
- state_up: float32 [1280, 5120], P('data', 'width'), may hold values from -1.75 to 1.75
- state_down: float32 [5120, 1280], P('width', 'data'), may hold values from -1.75 to 1.75
- state_query: float32 [1280, 1280], P('data', 'width'), may hold values from -1.75 to 1.75
- state_key: float32 [1280, 1280], P('data', 'width'), may hold values from -1.75 to 1.75
- state_value: float32 [1280, 1280], P('data', 'width'), may hold values from -1.75 to 1.75
- state_mixed: float32 [1280, 1280], P('width', 'data'), may hold values from -1.75 to 1.75
- state_norm: float32 [1280], P('data'), may hold values from -1.75 to 1.75
- state_bias: float32 [1280], P('data'), may hold values from -1.75 to 1.75
Outputs:
- half_up: bfloat16 [1280, 5120], P(None, 'width')
- half_down: bfloat16 [5120, 1280], P('width')
- half_query: bfloat16 [1280, 1280], P(None, 'width')
- half_key: bfloat16 [1280, 1280], P(None, 'width')
- half_value: bfloat16 [1280, 1280], P(None, 'width')
- half_mixed: bfloat16 [1280, 1280], P('width')
- half_norm: bfloat16 [1280], replicated
- half_bias: bfloat16 [1280], replicated
- next_up: float32 [1280, 5120], P('data', 'width')
- next_down: float32 [5120, 1280], P('width', 'data')
- next_query: float32 [1280, 1280], P('data', 'width')
- next_key: float32 [1280, 1280], P('data', 'width')
- next_value: float32 [1280, 1280], P('data', 'width')
- next_mixed: float32 [1280, 1280], P('width', 'data')
- next_norm: float32 [1280], P('data')
- next_bias: float32 [1280], P('data')
- state_new_up: float32 [1280, 5120], P('data', 'width')
- state_new_down: float32 [5120, 1280], P('width', 'data')
- state_new_query: float32 [1280, 1280], P('data', 'width')
- state_new_key: float32 [1280, 1280], P('data', 'width')
- state_new_value: float32 [1280, 1280], P('data', 'width')
- state_new_mixed: float32 [1280, 1280], P('width', 'data')
- state_new_norm: float32 [1280], P('data')
- state_new_bias: float32 [1280], P('data')
The draws below stay inside these ranges and needn't reach their ends.
All inputs are finite; a program needn't handle non-finite values.
Results may differ from the reference program's by a relative error of at most 0.0085.
Values may be sent and summed in bfloat16 or wider, within the bound.
No kernel may reach another device: no remote copies, remote signals or barrier semaphores. Data moves between devices by JAX's collectives and lax.ppermute only.
A program may use at most 128 MiB of HBM per device.

```python
import jax
import jax.numpy as jnp

WIDTH = 1280
INNER = 5120
ATTN = 1280
REPLICAS = 32


def with_spikes(result, stream_key, source, target, blocks, factor):
    def block_of(dim):
        return (jnp.arange(result.shape[dim]) // (result.shape[dim] // blocks)).reshape((-1,) + (1,) * (result.ndim - 1 - dim))

    near = jax.random.permutation(stream_key, blocks)[block_of(target)]
    second = (block_of(target) + blocks // 2) % blocks
    return jnp.where((block_of(source) == near) | (block_of(source) == second), factor * result, result)


def shard_levels(key, extent, shards, smallest, top_value):
    level, own = 1.0, jax.random.fold_in(key, 6)
    for axis_at, blocks in shards:
        draws = jnp.exp(jax.random.uniform(jax.random.fold_in(own, axis_at), (blocks,), jnp.float32, smallest / len(shards), top_value / len(shards)))
        level = level * jnp.repeat(draws, extent[axis_at] // blocks).reshape([-1 if axis == axis_at else 1 for axis in range(len(extent))])
    return level


def scatter_about(rng, shape, width, reach, split=(), dtype=jnp.bfloat16):
    factor_of = shard_levels(rng, shape, split, -0.22, 0.18) if split else 1.0
    drawn = jax.random.normal(rng, shape, jnp.float32) * width * factor_of
    return jnp.minimum(jnp.maximum(drawn, -reach), reach).astype(dtype)


def heavy_noise(own_key, extent, width, reach, cuts, heavy, dtype=jnp.bfloat16):
    entries = width * jax.random.normal(own_key, extent, jnp.float32)
    if cuts:
        entries = entries * shard_levels(own_key, extent, cuts, -0.22, 0.18)
    return jnp.clip(with_spikes(entries, jax.random.fold_in(own_key, 3), *heavy), -reach, reach).astype(dtype)


def setup_inputs(seed: int = 0) -> dict:
    splits = jax.random.split(jax.random.key(seed), 25)
    return {
        "slope_up": heavy_noise(splits[0], (REPLICAS, WIDTH, INNER), 0.1, 1.25, ((0, 32), (2, 8)), (0, 1, 32, 2.75), jnp.float32),
        "slope_down": heavy_noise(splits[1], (REPLICAS, INNER, WIDTH), 0.1, 1.25, ((0, 32), (1, 8)), (0, 2, 32, 2.75), jnp.float32),
        "slope_query": heavy_noise(splits[2], (REPLICAS, WIDTH, ATTN), 0.1, 1.25, ((0, 32), (2, 8)), (0, 1, 32, 2.75), jnp.float32),
        "slope_key": heavy_noise(splits[3], (REPLICAS, WIDTH, ATTN), 0.1, 1.25, ((0, 32), (2, 8)), (0, 1, 32, 2.75), jnp.float32),
        "slope_value": heavy_noise(splits[4], (REPLICAS, WIDTH, ATTN), 0.1, 1.25, ((0, 32), (2, 8)), (0, 1, 32, 2.75), jnp.float32),
        "slope_mixed": heavy_noise(splits[5], (REPLICAS, ATTN, WIDTH), 0.1, 1.25, ((0, 32), (1, 8)), (0, 2, 32, 2.75), jnp.float32),
        "slope_norm": heavy_noise(splits[6], (REPLICAS, WIDTH), 1.0, 12.0, ((0, 32),), (0, 1, 32, 2.75), jnp.float32),
        "slope_bias": heavy_noise(splits[7], (REPLICAS, WIDTH), 1.0, 12.0, ((0, 32),), (0, 1, 32, 2.75), jnp.float32),
        "param_up": scatter_about(splits[8], (WIDTH, INNER), WIDTH ** -0.5, 0.15625, ((0, 32), (1, 8)), jnp.float32),
        "param_down": scatter_about(splits[9], (INNER, WIDTH), INNER ** -0.5, 0.078125, ((0, 8), (1, 32)), jnp.float32),
        "param_query": scatter_about(splits[10], (WIDTH, ATTN), WIDTH ** -0.5, 0.15625, ((0, 32), (1, 8)), jnp.float32),
        "param_key": scatter_about(splits[11], (WIDTH, ATTN), WIDTH ** -0.5, 0.15625, ((0, 32), (1, 8)), jnp.float32),
        "param_value": scatter_about(splits[12], (WIDTH, ATTN), WIDTH ** -0.5, 0.15625, ((0, 32), (1, 8)), jnp.float32),
        "param_mixed": scatter_about(splits[13], (ATTN, WIDTH), ATTN ** -0.5, 0.15625, ((0, 8), (1, 32)), jnp.float32),
        "param_norm": jnp.clip(1.0 + 0.15 * jax.random.normal(splits[14], (WIDTH,), jnp.float32), 0.25, 1.75),
        "param_bias": scatter_about(splits[15], (WIDTH,), 0.5, 3.0, ((0, 32),), jnp.float32),
        "state_up": scatter_about(splits[16], (WIDTH, INNER), 0.3, 1.75, ((0, 32), (1, 8)), jnp.float32),
        "state_down": scatter_about(splits[17], (INNER, WIDTH), 0.3, 1.75, ((0, 8), (1, 32)), jnp.float32),
        "state_query": scatter_about(splits[18], (WIDTH, ATTN), 0.3, 1.75, ((0, 32), (1, 8)), jnp.float32),
        "state_key": scatter_about(splits[19], (WIDTH, ATTN), 0.3, 1.75, ((0, 32), (1, 8)), jnp.float32),
        "state_value": scatter_about(splits[20], (WIDTH, ATTN), 0.3, 1.75, ((0, 32), (1, 8)), jnp.float32),
        "state_mixed": scatter_about(splits[21], (ATTN, WIDTH), 0.3, 1.75, ((0, 8), (1, 32)), jnp.float32),
        "state_norm": scatter_about(splits[22], (WIDTH,), 0.3, 1.75, ((0, 32),), jnp.float32),
        "state_bias": scatter_about(splits[23], (WIDTH,), 0.3, 1.75, ((0, 32),), jnp.float32),
    }


learn_rate = 0.1
hold_rate = 0.8


def reference(slope_up, slope_down, slope_query, slope_key, slope_value, slope_mixed, slope_norm, slope_bias, param_up, param_down, param_query, param_key, param_value, param_mixed, param_norm, param_bias, state_up, state_down, state_query, state_key, state_value, state_mixed, state_norm, state_bias):
    mean_up = jnp.sum(slope_up.astype(jnp.float32), axis=0) * REPLICAS ** -0.5
    mean_down = jnp.sum(slope_down.astype(jnp.float32), axis=0) * REPLICAS ** -0.5
    mean_query = jnp.sum(slope_query.astype(jnp.float32), axis=0) * REPLICAS ** -0.5
    mean_key = jnp.sum(slope_key.astype(jnp.float32), axis=0) * REPLICAS ** -0.5
    mean_value = jnp.sum(slope_value.astype(jnp.float32), axis=0) * REPLICAS ** -0.5
    mean_mixed = jnp.sum(slope_mixed.astype(jnp.float32), axis=0) * REPLICAS ** -0.5
    mean_norm = jnp.sum(slope_norm.astype(jnp.float32), axis=0) * REPLICAS ** -0.5
    mean_bias = jnp.sum(slope_bias.astype(jnp.float32), axis=0) * REPLICAS ** -0.5
    state_new_up = hold_rate * state_up + mean_up
    next_up = param_up - learn_rate * state_new_up
    state_new_down = hold_rate * state_down + mean_down
    next_down = param_down - learn_rate * state_new_down
    state_new_query = hold_rate * state_query + mean_query
    next_query = param_query - learn_rate * state_new_query
    state_new_key = hold_rate * state_key + mean_key
    next_key = param_key - learn_rate * state_new_key
    state_new_value = hold_rate * state_value + mean_value
    next_value = param_value - learn_rate * state_new_value
    state_new_mixed = hold_rate * state_mixed + mean_mixed
    next_mixed = param_mixed - learn_rate * state_new_mixed
    state_new_norm = hold_rate * state_norm + mean_norm
    next_norm = param_norm - learn_rate * state_new_norm
    state_new_bias = hold_rate * state_bias + mean_bias
    next_bias = param_bias - learn_rate * state_new_bias
    half_up = next_up.astype(jnp.bfloat16)
    half_down = next_down.astype(jnp.bfloat16)
    half_query = next_query.astype(jnp.bfloat16)
    half_key = next_key.astype(jnp.bfloat16)
    half_value = next_value.astype(jnp.bfloat16)
    half_mixed = next_mixed.astype(jnp.bfloat16)
    half_norm = next_norm.astype(jnp.bfloat16)
    half_bias = next_bias.astype(jnp.bfloat16)
    return half_up, half_down, half_query, half_key, half_value, half_mixed, half_norm, half_bias, next_up, next_down, next_query, next_key, next_value, next_mixed, next_norm, next_bias, state_new_up, state_new_down, state_new_query, state_new_key, state_new_value, state_new_mixed, state_new_norm, state_new_bias
```

```python
import functools

import jax
import jax.numpy as jnp
from jax import lax
from jax.experimental import pallas as pl
from jax.experimental.pallas import tpu as pltpu
from jax.sharding import PartitionSpec as P

learn_rate = 0.1
hold_rate = 0.8


Z, ROWS = 8, 40
BF, F32 = jnp.bfloat16, jnp.float32
VM = pl.BlockSpec(memory_space=pltpu.VMEM)
SPLIT = 4 * ROWS


def to_z(step):
    return [(d, (d // 4 + step) % Z * 4 + d % 4) for d in range(32)]


TO_H = [(d, d ^ 2) for d in range(32)]
TO_C = [(d, d ^ 1) for d in range(32)]


def send(a, pairs):
    return lax.ppermute(a, "data", pairs)


def place():
    d = lax.axis_index("data")
    return d // 4, lax.rem(d // 2, 2), lax.rem(d, 2)


def call(body, outs, *args, scratch=(), limit=24 << 20, flops=1 << 20):
    moved = sum(a.size * a.dtype.itemsize for a in (*args, *outs))
    return pl.pallas_call(
        body,
        out_shape=outs,
        in_specs=[VM] * len(args),
        out_specs=[VM] * len(outs),
        scratch_shapes=scratch,
        compiler_params=pltpu.CompilerParams(vmem_limit_bytes=limit),
        cost_estimate=pl.CostEstimate(flops=flops, bytes_accessed=moved, transcendentals=0),
    )(*args)


def start_of(z, h, j, k):
    return lax.rem(z + j, Z) * SPLIT + jnp.where(h == k, 0, 2 * ROWS)


def deal(source, keep, give):
    z, h, c = place()
    for j in range(Z):
        for k in range(2):
            first = start_of(z, h, j, k)
            mine = pl.multiple_of(first + c * ROWS, 8)
            theirs = pl.multiple_of(first + (1 - c) * ROWS, 8)
            keep[j, k] = source[pl.ds(mine, ROWS), :].astype(BF)
            give[j, k] = source[pl.ds(theirs, ROWS), :].astype(BF)


def eye(n):
    return (
        lax.broadcasted_iota(jnp.int32, (n, n), 0) == lax.broadcasted_iota(jnp.int32, (n, n), 1)
    ).astype(BF)


def turned(a):
    return lax.dot_general(eye(a.shape[1]), a, (((1,), (1,)), ((), ())), preferred_element_type=F32)


def plain_in(up, keep, give):
    deal(up, keep, give)


def turned_in(down, keep, give, whole):
    for b in range(5):
        at = slice(b * 256, b * 256 + 256)
        whole[at, :] = turned(down[:, at].astype(BF))
    deal(whole, keep, give)


def stacked_in(query, key, value, mixed, norm, bias, keep, give, stack, whole):
    for n, ref in enumerate((query, key, value, mixed)):
        stack[n * 160 : n * 160 + 160, :] = ref[...]
    row = lax.broadcasted_iota(jnp.int32, (128, 1280), 0)
    stack[640:768, :] = jnp.where(row == 0, norm[...], jnp.where(row == 1, bias[...], 0.0))
    for b in range(5):
        at = slice(b * 256, b * 256 + 256)
        whole[at, :] = turned(stack[:, at].astype(BF))
    deal(whole, keep, give)


def blocks(columns):
    return [jax.ShapeDtypeStruct((Z, 2, ROWS, columns), BF)] * 2


def wide(a):
    return a.astype(F32)


def summed(keep, give):
    got = send(give, TO_C)

    def own(j, k):
        return wide(keep[j, k]) + wide(got[j, k])

    right = send(own(4, 0).astype(BF), to_z(1))
    left = send(own(4, 1).astype(BF), to_z(-1))
    right = jnp.stack([own(3, 0) + wide(right), own(3, 1)]).astype(BF)
    left = jnp.stack([own(5, 0), own(5, 1) + wide(left)]).astype(BF)
    for step in (2, 1):
        right, left = send(right, to_z(1)), send(left, to_z(-1))
        right = (wide(keep[step]) + wide(got[step]) + wide(right)).astype(BF)
        left = (wide(keep[8 - step]) + wide(got[8 - step]) + wide(left)).astype(BF)
    right, left = send(right, to_z(1)), send(left, to_z(-1))
    total = [own(0, k) + wide(right[k]) + wide(left[k]) for k in range(2)]
    return total[0] + wide(send(total[1].astype(BF), TO_H))


def gathered(own):
    pair = jnp.stack([own, send(own, TO_H)])
    parts = [((0, 0, 2), pair)]
    right = left = pair
    for step in (1, 2, 3):
        right, left = send(right, to_z(1)), send(left, to_z(-1))
        parts += [((8 - step, 0, 2), right), ((step, 0, 2), left)]
    parts += [((4, 0, 1), send(right[:1], to_z(1))), ((4, 1, 2), send(left[1:], to_z(-1)))]
    return parts + [(at, send(part, TO_C)) for at, part in parts], [at for at, _ in parts]


def settle(at, refs, target):
    z, h, c = place()
    for n, ref in enumerate(refs):
        j, low, high = at[n % len(at)]
        core = c if n < len(at) else 1 - c
        for k in range(low, high):
            row = pl.multiple_of(start_of(z, h, j, k) + core * ROWS, 8)
            target[pl.ds(row, ROWS), :] = ref[k - low].astype(target.dtype)


def plain_out(at, *refs):
    settle(at, refs[:-1], refs[-1])


def turned_out(at, *refs):
    *refs, out, whole = refs
    settle(at, refs, whole)
    for b in range(5):
        rows = slice(b * 128, b * 128 + 128)
        out[rows, :] = turned_rows(whole[:, rows]).astype(BF)


def turned_rows(a):
    return lax.dot_general(
        eye(a.shape[1]), a.astype(BF), (((1,), (1,)), ((), ())), preferred_element_type=F32
    )


def stacked_out(at, *refs):
    *refs, query, key, value, mixed, norm, bias, whole, stack = refs
    settle(at, refs, whole)
    for b in range(6):
        rows = slice(b * 128, b * 128 + 128)
        stack[rows, :] = turned_rows(whole[:, rows])
    for n, out in enumerate((query, key, value, mixed)):
        out[...] = stack[n * 160 : n * 160 + 160, :].astype(BF)
    norm[...] = stack[640:641, :].astype(BF)
    bias[...] = stack[641:642, :].astype(BF)


def step_of(total, param, state):
    state_new = hold_rate * state + total * 32**-0.5
    return param - learn_rate * state_new, state_new


def on_device(
    slope_up, slope_down, slope_query, slope_key, slope_value, slope_mixed, slope_norm, slope_bias,
    param_up, param_down, param_query, param_key, param_value, param_mixed, param_norm, param_bias,
    state_up, state_down, state_query, state_key, state_value, state_mixed, state_norm, state_bias,
):
    keep_u, give_u = call(plain_in, blocks(640), slope_up[0])
    keep_d, give_d = call(
        turned_in, blocks(640), slope_down[0], scratch=[pltpu.VMEM((1280, 640), F32)]
    )
    keep_q, give_q = call(
        stacked_in,
        blocks(768),
        slope_query[0].T, slope_key[0].T, slope_value[0].T, slope_mixed[0], slope_norm, slope_bias,
        scratch=[pltpu.VMEM((768, 1280), F32), pltpu.VMEM((1280, 768), F32)],
    )

    sum_u = summed(keep_u, give_u)
    next_up, state_new_up = step_of(sum_u, param_up, state_up)
    parts_u, at = gathered(next_up.astype(BF))
    sum_d = summed(keep_d, give_d)
    next_down, state_new_down = step_of(sum_d, param_down.T, state_down.T)
    parts_d, _ = gathered(next_down.astype(BF))
    sum_q = summed(keep_q, give_q)
    new = [
        step_of(sum_q[:, n * 160 : n * 160 + 160], param, state)
        for n, (param, state) in enumerate(
            (
                (param_query, state_query),
                (param_key, state_key),
                (param_value, state_value),
                (param_mixed.T, state_mixed.T),
            )
        )
    ]
    new += [
        step_of(sum_q[:, 640], param_norm, state_norm),
        step_of(sum_q[:, 641], param_bias, state_bias),
    ]
    halves = [n.astype(BF) for n, _ in new]
    halves = halves[:4] + [halves[4][:, None], halves[5][:, None], jnp.zeros((ROWS, 126), BF)]
    parts_q, _ = gathered(jnp.concatenate(halves, axis=1))

    def shape(*s):
        return jax.ShapeDtypeStruct(s, BF)

    (half_up,) = call(
        functools.partial(plain_out, at), [shape(1280, 640)], *[p for _, p in parts_u]
    )
    (half_down,) = call(
        functools.partial(turned_out, at), [shape(640, 1280)], *[p for _, p in parts_d],
        scratch=[pltpu.VMEM((1280, 640), F32)],
    )
    half_q, half_k, half_v, half_m, half_n, half_b = call(
        functools.partial(stacked_out, at),
        [shape(160, 1280)] * 4 + [shape(1, 1280)] * 2,
        *[p for _, p in parts_q],
        scratch=[pltpu.VMEM((1280, 768), F32), pltpu.VMEM((768, 1280), F32)],
    )
    nexts = [n for n, _ in new]
    states = [s for _, s in new]
    return (
        half_up, half_down, half_q.T, half_k.T, half_v.T, half_m, half_n[0], half_b[0],
        next_up, next_down.T, *nexts[:3], nexts[3].T, *nexts[4:],
        state_new_up, state_new_down.T, *states[:3], states[3].T, *states[4:],
    )


def solution(mesh):
    return jax.shard_map(
        on_device,
        mesh=mesh,
        in_specs=(
            P("data", None, "width"),
            P("data", "width", None),
            P("data", None, "width"),
            P("data", None, "width"),
            P("data", None, "width"),
            P("data", "width", None),
            P("data", None),
            P("data", None),
            *(
                P("data", "width"),
                P("width", "data"),
                P("data", "width"),
                P("data", "width"),
                P("data", "width"),
                P("width", "data"),
                P("data"),
                P("data"),
            )
            * 2,
        ),
        out_specs=(
            P(None, "width"),
            P("width", None),
            P(None, "width"),
            P(None, "width"),
            P(None, "width"),
            P("width", None),
            P(),
            P(),
            *(
                P("data", "width"),
                P("width", "data"),
                P("data", "width"),
                P("data", "width"),
                P("data", "width"),
                P("width", "data"),
                P("data"),
                P("data"),
            )
            * 2,
        ),
        check_vma=False,
    )
```

```python
import jax
import jax.numpy as jnp
from jax import lax
from jax.experimental import pallas as pl
from jax.experimental.pallas import tpu as pltpu
from jax.sharding import PartitionSpec as P

learn_rate = 0.1
hold_rate = 0.8


Z, ROWS = 8, 40
BF, F32 = jnp.bfloat16, jnp.float32
VM = pl.BlockSpec(memory_space=pltpu.VMEM)
SPLIT = 4 * ROWS


def to_z(step):
    return [(d, (d // 4 + step) % Z * 4 + d % 4) for d in range(32)]


TO_H = [(d, d ^ 2) for d in range(32)]
TO_C = [(d, d ^ 1) for d in range(32)]


def send(a, pairs):
    return lax.ppermute(a, "data", pairs)


def place():
    d = lax.axis_index("data")
    return d // 4, lax.rem(d // 2, 2), lax.rem(d, 2)


def call(body, outs, *args, scratch=(), limit=24 << 20, flops=1 << 20, far=0):
    moved = sum(a.size * a.dtype.itemsize for a in (*args, *outs))
    return pl.pallas_call(
        body,
        out_shape=outs,
        in_specs=[VM] * (len(args) - far) + [pl.BlockSpec(memory_space=pltpu.HBM)] * far,
        out_specs=[VM] * len(outs),
        scratch_shapes=scratch,
        compiler_params=pltpu.CompilerParams(vmem_limit_bytes=limit),
        cost_estimate=pl.CostEstimate(flops=flops, bytes_accessed=moved, transcendentals=0),
    )(*args)


def start_of(z, h, j, k):
    return lax.rem(z + j, Z) * SPLIT + jnp.where(h == k, 0, 2 * ROWS)


def deal(sources, keep, give):
    z, h, c = place()
    for j in range(Z):
        for k in range(2):
            first = start_of(z, h, j, k)
            mine = pl.multiple_of(first + c * ROWS, 8)
            theirs = pl.multiple_of(first + (1 - c) * ROWS, 8)
            at = 0
            for source in sources:
                to = slice(at, at + source.shape[1])
                keep[j, k, :, to] = source[pl.ds(mine, ROWS), :].astype(BF)
                give[j, k, :, to] = source[pl.ds(theirs, ROWS), :].astype(BF)
                at += source.shape[1]


def eye(n):
    return (
        lax.broadcasted_iota(jnp.int32, (n, n), 0) == lax.broadcasted_iota(jnp.int32, (n, n), 1)
    ).astype(BF)


def turned(a):
    return lax.dot_general(eye(a.shape[1]), a, (((1,), (1,)), ((), ())), preferred_element_type=F32)


def turn_in(refs, stack, whole):
    at = 0
    for ref in refs:
        stack[at : at + ref.shape[0], :] = ref[...].astype(BF)
        at += ref.shape[0]
    for b in range(5):
        strip = slice(b * 256, b * 256 + 256)
        whole[strip, :] = turned(stack[:, strip])


def first_in(*refs):
    sources, (keep, give), near = refs[:5], refs[5:7], refs[7:12]
    stack, whole, done = refs[12:]
    copies = [pltpu.make_async_copy(a, b, done.at[n]) for n, (a, b) in enumerate(zip(sources, near))]
    for copy in copies:
        copy.start()
    for copy in copies:
        copy.wait()
    up, query, key, norm, bias = near
    row = lax.broadcasted_iota(jnp.int32, (64, 1280), 0)
    ends = jnp.where(row == 0, norm[...], jnp.where(row == 1, bias[...], 0.0))
    turn_in((query, key, ends), stack, whole)
    deal((up, whole), keep, give)


def second_in(down, value, mixed, keep, give, stack, whole):
    turn_in((down, value, mixed, jnp.zeros((64, 1280), BF)), stack, whole)
    deal((whole,), keep, give)


def wide(a):
    return a.astype(F32)


def summed(keep, give, way):
    got = send(give, TO_C)

    def own(j):
        return wide(keep[j % Z]) + wide(got[j % Z])

    long, short = own(4 * way).astype(BF), own(-3 * way).astype(BF)
    for step in (3, 2, 1):
        mark = long
        long = (own(step * way) + wide(send(long, to_z(way)))).astype(BF)
        short = send(short, to_z(-way))
        if step > 1:
            short = (own((1 - step) * way) + wide(short)).astype(BF)
    return (own(0) + wide(send(long, to_z(way))) + wide(short)).astype(BF), mark


def column(row):
    return jnp.sum(jnp.where(diagonal(), row, 0.0), axis=1, keepdims=True)


def diagonal():
    square = (ROWS, ROWS)
    return lax.broadcasted_iota(jnp.int32, square, 0) == lax.broadcasted_iota(jnp.int32, square, 1)


def hold_first(*refs):
    *refs, _, held = refs
    held[...] = jnp.zeros_like(held)
    for n, (up, query, key, norm, bias) in enumerate((refs[:5], refs[5:])):
        held[n, :, 0:640] = up[...]
        held[n, :, 640:800] = query[...]
        held[n, :, 800:960] = key[...]
        held[n, :, 960:961] = column(norm[...])
        held[n, :, 961:962] = column(bias[...])


def hold_second(*refs):
    *refs, _, held = refs
    held[...] = jnp.zeros_like(held)
    for n, (down, value, mixed) in enumerate((refs[:3], refs[3:])):
        held[n, :, 0:640] = down[...]
        held[n, :, 640:800] = value[...]
        held[n, :, 800:960] = mixed[...]


def update(pair, other, own, theirs, half, fresh):
    for k, held in ((0, own), (1, theirs)):
        total = wide(pair[k]) + wide(other[1 - k])
        state_new = hold_rate * held[1] + total * 32**-0.5
        following = held[0] - learn_rate * state_new
        half[k] = following.astype(BF)
        if k == 0:
            fresh[0], fresh[1] = following, state_new


def release_first(fresh, *outs):
    for n, (up, query, key, norm, bias) in enumerate((outs[:5], outs[5:])):
        up[...] = fresh[n, :, 0:640]
        query[...] = fresh[n, :, 640:800]
        key[...] = fresh[n, :, 800:960]
        norm[...] = jnp.sum(jnp.where(diagonal(), fresh[n, :, 960:961], 0.0), axis=0, keepdims=True)
        bias[...] = jnp.sum(jnp.where(diagonal(), fresh[n, :, 961:962], 0.0), axis=0, keepdims=True)


def release_second(fresh, *outs):
    for n, (down, value, mixed) in enumerate((outs[:3], outs[3:])):
        down[...] = fresh[n, :, 0:640]
        value[...] = fresh[n, :, 640:800]
        mixed[...] = fresh[n, :, 800:960]


def renewed(pair, held):
    return call(
        update,
        [shaped(2, ROWS, 1024), shaped(2, ROWS, 1024, dtype=F32)],
        pair, send(pair, TO_H), held, send(held, TO_H),
    )


def shaped(*s, dtype=BF):
    return jax.ShapeDtypeStruct(s, dtype)


def pack(*refs):
    for n, ref in enumerate(refs[:-1]):
        refs[-1][n] = ref[...]


def packed(arrays):
    return call(pack, [shaped(len(arrays), *arrays[0].shape)], *arrays)[0]


def gathered(pair, way):
    long, short = [pair], [pair]
    for _ in range(4):
        long.append(send(long[-1], to_z(way)))
    for _ in range(3):
        short.append(send(short[-1], to_z(-way)))
    early = [pair, long[1], short[1], long[2], short[2]]
    late = [long[3], short[3], long[4]]
    return (*early, *late, send(packed(early), TO_C), send(packed(late), TO_C))


def settle(way, refs, targets):
    z, h, c = place()
    steps = [n % Z for n in (0, -way, way, -2 * way, 2 * way, -3 * way, 3 * way, 4)]
    for n, j in enumerate(steps):
        for k in range(2):
            for core, block in ((c, refs[n].at[k]), (1 - c, refs[8 + n // 5].at[n % 5, k])):
                row = pl.multiple_of(start_of(z, h, j, k) + core * ROWS, 8)
                at = 0
                for target in targets:
                    width = target.shape[1]
                    target[pl.ds(row, ROWS), :] = block[:, at : at + width].astype(target.dtype)
                    at += width


def turn_back(whole, stack):
    for n in range(0, whole.shape[1], 128):
        stack[n : n + 128, :] = turned(whole[:, n : n + 128].astype(BF)).astype(BF)


def first_out(*refs):
    *refs, up, query, key, norm, bias, whole, stack = refs
    settle(1, refs, (up, whole))
    turn_back(whole, stack)
    query[...] = stack[0:160, :]
    key[...] = stack[160:320, :]
    norm[...] = stack[320:321, :]
    bias[...] = stack[321:322, :]


def second_out(*refs):
    *refs, down, value, mixed, whole, stack = refs
    settle(-1, refs, (whole,))
    turn_back(whole, stack)
    down[...] = stack[0:640, :]
    value[...] = stack[640:800, :]
    mixed[...] = stack[800:960, :]


def on_device(
    slope_up, slope_down, slope_query, slope_key, slope_value, slope_mixed, slope_norm, slope_bias,
    param_up, param_down, param_query, param_key, param_value, param_mixed, param_norm, param_bias,
    state_up, state_down, state_query, state_key, state_value, state_mixed, state_norm, state_bias,
):
    dealt = [shaped(Z, 2, ROWS, 1024)] * 2
    near = [(1280, 640), (160, 1280), (160, 1280), (1, 1280), (1, 1280)]
    keep_a, give_a = call(
        first_in, dealt,
        slope_up[0], slope_query[0].T, slope_key[0].T, slope_norm, slope_bias,
        scratch=[
            *(pltpu.VMEM(s, F32) for s in near),
            pltpu.VMEM((384, 1280), BF),
            pltpu.VMEM((1280, 384), F32),
            pltpu.SemaphoreType.DMA((5,)),
        ],
        far=5,
    )
    keep_b, give_b = call(
        second_in, dealt,
        slope_down[0], slope_value[0].T, slope_mixed[0],
        scratch=[pltpu.VMEM((1024, 1280), BF), pltpu.VMEM((1280, 1024), F32)],
    )
    pair_a, mark_a = summed(keep_a, give_a, 1)
    pair_b, mark_b = summed(keep_b, give_b, -1)
    both = [shaped(2, ROWS, 1024, dtype=F32)]
    (held_a,) = call(
        hold_first, both,
        param_up, param_query, param_key, param_norm[None], param_bias[None],
        state_up, state_query, state_key, state_norm[None], state_bias[None],
        mark_a, far=1,
    )
    (held_b,) = call(
        hold_second, both,
        param_down.T, param_value, param_mixed.T, state_down.T, state_value, state_mixed.T,
        mark_b, far=1,
    )
    half_a, fresh_a = renewed(pair_a, held_a)
    parts_a = gathered(half_a, 1)
    half_b, fresh_b = renewed(pair_b, held_b)
    parts_b = gathered(half_b, -1)

    def rows(*widths):
        return [shaped(ROWS, w, dtype=F32) if w else shaped(1, ROWS, dtype=F32) for w in widths] * 2

    new_a = call(release_first, rows(640, 160, 160, 0, 0), fresh_a)
    new_b = call(release_second, rows(640, 160, 160), fresh_b)

    half_up, half_q, half_k, half_n, half_b = call(
        first_out,
        [shaped(1280, 640), *[shaped(160, 1280)] * 2, *[shaped(1, 1280)] * 2],
        *parts_a,
        scratch=[pltpu.VMEM((1280, 384), F32), pltpu.VMEM((384, 1280), BF)],
    )
    half_down, half_v, half_m = call(
        second_out,
        [shaped(640, 1280), *[shaped(160, 1280)] * 2],
        *parts_b,
        scratch=[pltpu.VMEM((1280, 1024), F32), pltpu.VMEM((1024, 1280), BF)],
    )

    def ordered(a, b):
        up, query, key, norm, bias = a
        down, value, mixed = b
        return up, down.T, query, key, value, mixed.T, norm[0], bias[0]

    return (
        half_up, half_down, half_q.T, half_k.T, half_v.T, half_m, half_n[0], half_b[0],
        *ordered(new_a[:5], new_b[:3]),
        *ordered(new_a[5:], new_b[3:]),
    )


def solution(mesh):
    return jax.shard_map(
        on_device,
        mesh=mesh,
        in_specs=(
            P("data", None, "width"),
            P("data", "width", None),
            P("data", None, "width"),
            P("data", None, "width"),
            P("data", None, "width"),
            P("data", "width", None),
            P("data", None),
            P("data", None),
            *(
                P("data", "width"),
                P("width", "data"),
                P("data", "width"),
                P("data", "width"),
                P("data", "width"),
                P("width", "data"),
                P("data"),
                P("data"),
            )
            * 2,
        ),
        out_specs=(
            P(None, "width"),
            P("width", None),
            P(None, "width"),
            P(None, "width"),
            P(None, "width"),
            P("width", None),
            P(),
            P(),
            *(
                P("data", "width"),
                P("width", "data"),
                P("data", "width"),
                P("data", "width"),
                P("data", "width"),
                P("width", "data"),
                P("data"),
                P("data"),
            )
            * 2,
        ),
        check_vma=False,
    )
```

```python
import functools

import jax
import jax.numpy as jnp
from jax import lax
from jax.experimental import pallas as pl
from jax.experimental.pallas import tpu as pltpu
from jax.sharding import PartitionSpec as P


learn_rate = 0.1
hold_rate = 0.8


Z, ROWS = 8, 40
BF, F32 = jnp.bfloat16, jnp.float32
VM = pl.BlockSpec(memory_space=pltpu.VMEM)
SPLIT = 4 * ROWS


def to_z(step):
    return [(d, (d // 4 + step) % Z * 4 + d % 4) for d in range(32)]


TO_H = [(d, d ^ 2) for d in range(32)]
TO_C = [(d, d ^ 1) for d in range(32)]


def send(a, pairs):
    return lax.ppermute(a, "data", pairs)


def place():
    d = lax.axis_index("data")
    return d // 4, lax.rem(d // 2, 2), lax.rem(d, 2)


def call(body, outs, *args, scratch=(), flops=1 << 20, far=0, out_space=pltpu.VMEM):
    moved = sum(a.size * a.dtype.itemsize for a in (*args, *outs))
    near = len(args) - far
    args = (*args[:near], *(pltpu.with_memory_space_constraint(a, pltpu.HBM) for a in args[near:]))
    return pl.pallas_call(
        body,
        out_shape=outs,
        in_specs=[VM] * near + [pl.BlockSpec(memory_space=pltpu.HBM)] * far,
        out_specs=[pl.BlockSpec(memory_space=out_space)] * len(outs),
        scratch_shapes=scratch,
        compiler_params=pltpu.CompilerParams(vmem_limit_bytes=24 << 20),
        cost_estimate=pl.CostEstimate(flops=flops, bytes_accessed=moved, transcendentals=0),
    )(*args)


def start_of(z, h, j, k):
    return lax.rem(z + j, Z) * SPLIT + jnp.where(h == k, 0, 2 * ROWS)


def deal(sources, keep, give):
    z, h, c = place()
    for j in range(Z):
        for k in range(2):
            first = start_of(z, h, j, k)
            mine = pl.multiple_of(first + c * ROWS, 8)
            theirs = pl.multiple_of(first + (1 - c) * ROWS, 8)
            at = 0
            for source in sources:
                to = slice(at, at + source.shape[1])
                keep[j, k, :, to] = source[pl.ds(mine, ROWS), :].astype(BF)
                give[j, k, :, to] = source[pl.ds(theirs, ROWS), :].astype(BF)
                at += source.shape[1]


def eye(n):
    return (
        lax.broadcasted_iota(jnp.int32, (n, n), 0) == lax.broadcasted_iota(jnp.int32, (n, n), 1)
    ).astype(BF)


def turned(a):
    return lax.dot_general(eye(a.shape[1]), a, (((1,), (1,)), ((), ())), preferred_element_type=F32)


def turn_in(refs, stack, whole):
    at = 0
    for ref in refs:
        stack[at : at + ref.shape[0], :] = ref[...].astype(BF)
        at += ref.shape[0]
    for b in range(5):
        strip = slice(b * 256, b * 256 + 256)
        whole[strip, :] = turned(stack[:, strip])


def copies(sources, near, done):
    started = [
        pltpu.make_async_copy(a, b, done.at[n]) for n, (a, b) in enumerate(zip(sources, near))
    ]
    for copy in started:
        copy.start()
    return started


def first_in(*refs):
    sources, (keep, give), near = refs[:5], refs[5:7], refs[7:12]
    stack, whole, done = refs[12:]
    started = copies(sources, near, done)
    for copy in started[:4]:
        copy.wait()
    query, key, norm, bias, up = near
    row = lax.broadcasted_iota(jnp.int32, (64, 1280), 0)
    ends = jnp.where(row == 0, norm[...], jnp.where(row == 1, bias[...], 0.0))
    turn_in((query, key, ends), stack, whole)
    started[4].wait()
    deal((up, whole), keep, give)


def second_in(down, value, mixed, keep, give, stack, whole):
    turn_in((down, value, mixed, jnp.zeros((64, 1280), BF)), stack, whole)
    deal((whole,), keep, give)


def wide(a):
    return a.astype(F32)


def add_first(long_at, short_at, keep, got, long, short):
    long[...] = (wide(keep[long_at]) + wide(got[long_at])).astype(BF)
    short[...] = (wide(keep[short_at]) + wide(got[short_at])).astype(BF)


def add(at, keep, got, *refs):
    *came, out = refs
    total = wide(keep[at]) + wide(got[at])
    for ref in came:
        total = total + wide(ref[...])
    out[...] = total.astype(BF)


def summed(keep, give, way):
    got = send(give, TO_C)
    block = shaped(2, ROWS, 1024)
    first = functools.partial(add_first, 4, -3 * way % Z)
    long, short = call(first, [block] * 2, keep, got)

    def plus(j, *came):
        return call(functools.partial(add, j % Z), [block], keep, got, *came)[0]

    for step in (3, 2, 1):
        long = send(long, to_z(way))
        short = send(short, to_z(-way))
        long = plus(step * way, long)
        if step > 1:
            short = plus((1 - step) * way, short)
    return plus(0, send(long, to_z(way)), short)


def column(row):
    return jnp.sum(jnp.where(diagonal(), row, 0.0), axis=1, keepdims=True)


def diagonal():
    square = (ROWS, ROWS)
    return lax.broadcasted_iota(jnp.int32, square, 0) == lax.broadcasted_iota(jnp.int32, square, 1)


def hold(*refs):
    *refs, held = refs
    held[...] = jnp.zeros_like(held)
    for n in range(2):
        up, down, query, key, value, mixed, norm, bias = refs[8 * n : 8 * n + 8]
        held[n, :, 0:640] = up[...]
        held[n, :, 640:800] = query[...]
        held[n, :, 800:960] = key[...]
        held[n, :, 960:961] = column(norm[...])
        held[n, :, 961:962] = column(bias[...])
        held[2 + n, :, 0:640] = down[...]
        held[2 + n, :, 640:800] = value[...]
        held[2 + n, :, 800:960] = mixed[...]


def update(at, pair, other, own, theirs, half, fresh):
    for k, held in ((0, own), (1, theirs)):
        total = wide(pair[k]) + wide(other[1 - k])
        state_new = hold_rate * held[at + 1] + total * 32**-0.5
        following = held[at] - learn_rate * state_new
        half[k] = following.astype(BF)
        if k == 0:
            fresh[0], fresh[1] = following, state_new


def release_first(fresh, *outs):
    for n, (up, query, key, norm, bias) in enumerate((outs[:5], outs[5:])):
        up[...] = fresh[n, :, 0:640]
        query[...] = fresh[n, :, 640:800]
        key[...] = fresh[n, :, 800:960]
        norm[...] = jnp.sum(jnp.where(diagonal(), fresh[n, :, 960:961], 0.0), axis=0, keepdims=True)
        bias[...] = jnp.sum(jnp.where(diagonal(), fresh[n, :, 961:962], 0.0), axis=0, keepdims=True)


def release_second(fresh, *outs):
    for n, (down, value, mixed) in enumerate((outs[:3], outs[3:])):
        down[...] = fresh[n, :, 0:640]
        value[...] = fresh[n, :, 640:800]
        mixed[...] = fresh[n, :, 800:960]


def shaped(*s, dtype=BF):
    return jax.ShapeDtypeStruct(s, dtype)


def pack(release, *refs):
    blocks, fresh, (out, *outs) = refs[:7], refs[7], refs[8:]
    for n, block in enumerate(blocks):
        out[n] = block[...]
    release(fresh, *outs)


def gathered(pair, way, release, fresh, outs):
    long, short = [pair], [pair]
    for n in range(4):
        long.append(send(long[-1], to_z(way)))
        if n < 3:
            short.append(send(short[-1], to_z(-way)))
    early = [pair, long[1], short[1], long[2], short[2], long[3], short[3]]
    together, *new = call(
        functools.partial(pack, release), [shaped(7, 2, ROWS, 1024), *outs], *early, fresh
    )
    swapped = send(together, TO_C), send(long[4], TO_C)
    return (*early, long[4], *swapped), new


def settle(way, refs, targets):
    z, h, c = place()
    steps = [n % Z for n in (0, -way, way, -2 * way, 2 * way, -3 * way, 3 * way, 4)]
    for n, j in enumerate(steps):
        for k in range(2):
            other = refs[8].at[n, k] if n < 7 else refs[9].at[k]
            for core, block in ((c, refs[n].at[k]), (1 - c, other)):
                row = pl.multiple_of(start_of(z, h, j, k) + core * ROWS, 8)
                at = 0
                for target in targets:
                    width = target.shape[1]
                    target[pl.ds(row, ROWS), :] = block[:, at : at + width].astype(target.dtype)
                    at += width


def turn_back(whole, stack):
    for n in range(0, whole.shape[1], 256):
        strip = slice(n, min(n + 256, whole.shape[1]))
        stack[strip, :] = turned(whole[:, strip].astype(BF)).astype(BF)


def first_out(*refs):
    *refs, up, query, key, norm, bias, whole, stack = refs
    settle(1, refs, (up, whole))
    turn_back(whole, stack)
    query[...] = stack[0:160, :]
    key[...] = stack[160:320, :]
    norm[...] = stack[320, :]
    bias[...] = stack[321, :]


def second_out(*refs):
    *refs, down, value, mixed, whole, stack, done = refs
    settle(-1, refs, (whole,))
    moves = [(slice(n, n + 128), down.at[n : n + 128]) for n in range(0, 640, 128)]
    moves += [(slice(640, 800), value), (slice(800, 960), mixed)]
    copies = [
        pltpu.make_async_copy(stack.at[rows], to, done.at[n]) for n, (rows, to) in enumerate(moves)
    ]
    started = 0
    for strip in range(0, 1024, 128):
        to = slice(strip, strip + 128)
        stack[to, :] = turned(whole[:, to].astype(BF)).astype(BF)
        while started < 7 and moves[started][0].stop <= strip:
            copies[started].start()
            started += 1
    copies[6].start()
    for copy in copies:
        copy.wait()


def on_device(
    slope_up, slope_down, slope_query, slope_key, slope_value, slope_mixed, slope_norm, slope_bias,
    param_up, param_down, param_query, param_key, param_value, param_mixed, param_norm, param_bias,
    state_up, state_down, state_query, state_key, state_value, state_mixed, state_norm, state_bias,
):
    dealt = [shaped(Z, 2, ROWS, 1024)] * 2

    def stacks(rows):
        return [pltpu.VMEM((rows, 1280), BF), pltpu.VMEM((1280, rows), F32)]

    slopes = slope_query[0].T, slope_key[0].T, slope_norm, slope_bias, slope_up[0]
    near = [pltpu.VMEM(a.shape, F32) for a in slopes]
    done = pltpu.SemaphoreType.DMA((5,))
    keep_a, give_a = call(first_in, dealt, *slopes, scratch=[*near, *stacks(384), done], far=5)
    slopes = slope_down[0], slope_value[0].T, slope_mixed[0]
    keep_b, give_b = call(second_in, dealt, *slopes, scratch=stacks(1024))
    pair_a = summed(keep_a, give_a, 1)
    pair_b = summed(keep_b, give_b, -1)
    (held,) = call(
        hold, [shaped(4, ROWS, 1024, dtype=F32)],
        param_up, param_down.T, param_query, param_key, param_value, param_mixed.T,
        param_norm[None], param_bias[None],
        state_up, state_down.T, state_query, state_key, state_value, state_mixed.T,
        state_norm[None], state_bias[None],
    )
    theirs = send(held, TO_H)

    def renewed(pair, at):
        other = send(pair, TO_H)
        return call(
            functools.partial(update, at),
            [shaped(2, ROWS, 1024), shaped(2, ROWS, 1024, dtype=F32)],
            pair, other, held, theirs,
        )

    def rows(*widths):
        return [shaped(ROWS, w, dtype=F32) if w else shaped(1, ROWS, dtype=F32) for w in widths] * 2

    half_a, fresh_a = renewed(pair_a, 0)
    parts_a, new_a = gathered(half_a, 1, release_first, fresh_a, rows(640, 160, 160, 0, 0))
    half_b, fresh_b = renewed(pair_b, 2)
    parts_b, new_b = gathered(half_b, -1, release_second, fresh_b, rows(640, 160, 160))

    half_up, half_q, half_k, half_n, half_b = call(
        first_out,
        [shaped(1280, 640), *[shaped(160, 1280)] * 2, *[shaped(1280)] * 2],
        *parts_a,
        scratch=[pltpu.VMEM((1280, 384), F32), pltpu.VMEM((384, 1280), BF)],
    )
    half_down, half_v, half_m = call(
        second_out,
        [shaped(640, 1280), *[shaped(160, 1280)] * 2],
        *parts_b,
        scratch=[
            pltpu.VMEM((1280, 1024), F32),
            pltpu.VMEM((1024, 1280), BF),
            pltpu.SemaphoreType.DMA((7,)),
        ],
        out_space=pltpu.HBM,
    )

    def ordered(a, b):
        up, query, key, norm, bias = a
        down, value, mixed = b
        return up, down.T, query, key, value, mixed.T, norm[0], bias[0]

    return (
        half_up, half_down, half_q.T, half_k.T, half_v.T, half_m, half_n, half_b,
        *ordered(new_a[:5], new_b[:3]),
        *ordered(new_a[5:], new_b[3:]),
    )


def solution(mesh):
    return jax.shard_map(
        on_device,
        mesh=mesh,
        in_specs=(
            P("data", None, "width"),
            P("data", "width", None),
            P("data", None, "width"),
            P("data", None, "width"),
            P("data", None, "width"),
            P("data", "width", None),
            P("data", None),
            P("data", None),
            *(
                P("data", "width"),
                P("width", "data"),
                P("data", "width"),
                P("data", "width"),
                P("data", "width"),
                P("width", "data"),
                P("data"),
                P("data"),
            )
            * 2,
        ),
        out_specs=(
            P(None, "width"),
            P("width", None),
            P(None, "width"),
            P(None, "width"),
            P(None, "width"),
            P("width", None),
            P(),
            P(),
            *(
                P("data", "width"),
                P("width", "data"),
                P("data", "width"),
                P("data", "width"),
                P("data", "width"),
                P("width", "data"),
                P("data"),
                P("data"),
            )
            * 2,
        ),
        check_vma=False,
    )
```
